128 devices in a mesh: freq: 4 (over x_hi, core), gblk: 32 (over x_lo, z, y).
Axes of the slice: x: 4 (x_hi: 2, x_lo: 2; x = x_hi * 2 + x_lo), y: 4, z: 4, core: 2. Of those that a mesh axis runs over, the one named last changes fastest.
Arguments:
- w_imag: bfloat16 [8, 8192, 16384], P('freq', 'gblk'), may hold values from -0.046875 to 0.046875
- w_real: bfloat16 [4, 8192, 16384], P('freq', 'gblk'), may hold values from -0.046875 to 0.046875
- pair_elements: bfloat16 [8192, 256], P('gblk'), may hold values from -1 to 1
- quad_weight: float32 [8, 128], P('freq'), may hold values from 0.1 to 1
- residue_freq: int32 [128], replicated, may hold values from 0 to 3
- owner_bands: int32 [128], replicated, may hold values from 0 to 127, each once
Outputs:
- sigma: float32 [128, 256], P(('freq', 'gblk'))
The draws below stay inside these ranges and needn't reach their ends.
Inputs may be any that keep to these rules, and one draw needn't show every extreme that they name: `owner_bands`: each band appears once.
All inputs are finite; a program needn't handle non-finite values.
Results may differ from the reference program's by a relative error of at most 0.0003.
Values may be sent and summed in bfloat16 or wider, within the bound.
No kernel may reach another device: no remote copies, remote signals or barrier semaphores. Data moves between devices by JAX's collectives and lax.ppermute only.
A program may use at most 128 MiB of HBM per device.

```python
import math
import jax
import jax.numpy as jnp
from jax import lax

NG = 8192
NB = 128
NFI = 8
NFR = 4


def set_ends(result, stream_key, low, top_value):
    longest = result.shape.index(max(result.shape))
    spots = []
    for shift in (0, 1):
        where = [jax.random.randint(jax.random.fold_in(stream_key, axis), (), 0, length) for axis, length in enumerate(result.shape)]
        where[longest] = (where[longest] + shift) % result.shape[longest]
        spots.append(tuple(where))
    return result.at[spots[0]].set(low).at[spots[1]].set(top_value)


def strengthened(values, stream_key, source, target, blocks, factor):
    owner, partner = [(jnp.arange(values.shape[position]) // (values.shape[position] // blocks)).reshape([-1 if axis == position else 1 for axis in range(values.ndim)]) for position in (source, target)]
    chosen = jax.random.permutation(stream_key, blocks)[partner]
    strong = (owner == chosen) | (owner == (partner + blocks // 2) % blocks)
    return jnp.where(strong, factor * values, values)


def block_scale(stream_key, extent, shards, smallest, largest):
    def one(dim, parts):
        steps = jax.random.uniform(jax.random.fold_in(jax.random.fold_in(stream_key, 6), dim), (parts,), jnp.float32, smallest / len(shards), largest / len(shards))
        return jnp.repeat(jnp.exp(steps), extent[dim] // parts).reshape((-1,) + (1,) * (len(extent) - dim - 1))

    factor_of = one(*shards[0])
    for cut in shards[1:]:
        factor_of = factor_of * one(*cut)
    return factor_of


def scatter_about(rng, dims, spread, reach, split=(), held_as=jnp.bfloat16):
    loudness = block_scale(rng, dims, split, -0.22, 0.18) if split else 1.0
    entries = jax.random.normal(rng, dims, jnp.float32) * spread * loudness
    return jnp.minimum(jnp.maximum(entries, -reach), reach).astype(held_as)


def noise_with(rng, dims, scale, limit, cuts, heavy, kind=jnp.bfloat16):
    drawn = scale * jax.random.normal(rng, dims, jnp.float32)
    if cuts:
        drawn = drawn * block_scale(rng, dims, cuts, -0.22, 0.18)
    return jnp.clip(strengthened(drawn, jax.random.fold_in(rng, 3), *heavy), -limit, limit).astype(kind)


def setup_inputs(seed: int = 0) -> dict:
    keys = jax.random.split(jax.random.key(seed), 7)
    w_imag = scatter_about(keys[0], (NFI, NG, 2 * NG), (2 * NG) ** -0.5, 0.046875, ((0, 4), (1, 32)))
    w_real = scatter_about(keys[1], (NFR, NG, 2 * NG), (2 * NG) ** -0.5, 0.046875, ((0, 4), (1, 32)))
    pair_elements = noise_with(keys[2], (NG, 2 * NB), 0.09, 1.0, ((0, 32),), (0, 1, 32, 2.75))
    quad_weight = jnp.clip(jnp.exp(math.log(1.0) - 2.3025851 * jax.random.uniform(keys[3], (NFI, NB), jnp.float32) ** block_scale(keys[3], (NFI, NB), ((0, 4),), -0.2, 0.2)), 0.1, 1.0)
    residue_freq = set_ends(jax.random.randint(keys[4], (NB,), 0, NFR), jax.random.fold_in(keys[4], 1), 0, NFR - 1).astype(jnp.int32)
    owner_bands = jax.random.permutation(keys[5], NB).astype(jnp.int32)
    return {"w_imag": w_imag, "w_real": w_real, "pair_elements": pair_elements, "quad_weight": quad_weight, "residue_freq": residue_freq, "owner_bands": owner_bands}


def reference(w_imag, w_real, pair_elements, quad_weight, residue_freq, owner_bands):
    bands = NB
    real_part = pair_elements[:, :bands]
    imag_part = pair_elements[:, bands:]
    lower_rows = jnp.concatenate([-imag_part, real_part], axis=1)
    stacked = jnp.concatenate([pair_elements, lower_rows], axis=0).astype(jnp.float32)
    block_rows = min(NG, 1024)
    wide_elems = pair_elements.astype(jnp.float32).reshape(NG // block_rows, block_rows, 2 * bands)

    def per_frequency(matrix):
        pieces = matrix.reshape(NG // block_rows, block_rows, 2 * NG)

        def per_block(packed):
            w_block, m_block = packed
            x_block = jnp.dot(w_block.astype(jnp.float32), stacked, precision=lax.Precision.HIGHEST)
            return jnp.dot(m_block.T, x_block, precision=lax.Precision.HIGHEST)

        blocks = jnp.sum(lax.map(per_block, (pieces, wide_elems)), axis=0)
        sig_re = blocks[:bands, :bands] + blocks[bands:, bands:]
        sig_im = blocks[:bands, bands:] - blocks[bands:, :bands]
        return jnp.concatenate([sig_re, sig_im], axis=1)

    s_imag = lax.map(per_frequency, w_imag)
    s_real = lax.map(per_frequency, w_real)
    residue_weight = (residue_freq[None, :] == jnp.arange(NFR, dtype=jnp.int32)[:, None]).astype(jnp.float32)
    total = jnp.sum(quad_weight[:, :, None] * s_imag, axis=0) + jnp.sum(residue_weight[:, :, None] * s_real, axis=0)
    return total[owner_bands]
```

```python
import functools
import jax
import jax.numpy as jnp
from jax import lax
from jax.experimental import pallas as pl
from jax.experimental.pallas import tpu as pltpu
from jax.sharding import Mesh
from jax.sharding import PartitionSpec as P


NAMES = ("xh", "c", "xl", "z", "y")
PLANE = ("c", "xl", "z", "y")
ALL = NAMES
COLS = 1024
FIRST = 3
NEAR = (0, 1, 3, 2)
FAR = (0, 1, 3, 2)


def device_id(xl, c, z, y):
    return ((c * 2 + xl) * 4 + z % 4) * 4 + y % 4


def moved(x, target):
    pairs = []
    for xl in range(2):
        for c in range(2):
            for z in range(4):
                for y in range(4):
                    to = target(xl, c, z, y)
                    if to is not None:
                        pairs.append((device_id(xl, c, z, y), device_id(*to)))
    return lax.ppermute(x, PLANE, pairs)


def to_class_core(x, k):
    def target(xl, c, z, y):
        if c == xl and k == 0:
            return None
        at = xl if c == xl else 1 - xl
        return (at, xl, z, y + k) if xl == 0 else (at, xl, z + k, y)

    return moved(x, target)


def along_other(x, k):
    return moved(x, lambda xl, c, z, y: (xl, c, z + k, y) if c == 0 else (xl, c, z, y + k))


def other_core(x):
    return moved(x, lambda xl, c, z, y: (xl, 1 - c, z, y))


def prep_kernel(at_ref, m_ref, owner_ref, residue_ref, quad_ref, l_ref, q_ref):
    nb = owner_ref.shape[1]
    owner = jnp.broadcast_to(owner_ref[...].astype(jnp.float32), (nb, nb)).T
    lanes = lax.broadcasted_iota(jnp.int32, (nb, nb), 1)
    pick = (owner.astype(jnp.int32) == lanes).astype(jnp.float32)
    pick16 = pick.astype(jnp.bfloat16)
    nt = (((1,), (1,)), ((), ()))
    g = m_ref.shape[0]
    re = lax.dot_general(pick16, m_ref[:, :nb], nt, preferred_element_type=jnp.float32)
    im = lax.dot_general(pick16, m_ref[:, nb:], nt, preferred_element_type=jnp.float32)
    l_ref[:nb, :g] = re.astype(jnp.bfloat16)
    l_ref[:nb, g:] = im.astype(jnp.bfloat16)
    l_ref[nb:, :g] = (-im).astype(jnp.bfloat16)
    l_ref[nb:, g:] = re.astype(jnp.bfloat16)
    nq = quad_ref.shape[0]
    fid = at_ref[4]
    rows = [quad_ref[f : f + 1, :] for f in range(nq)]
    for r in range(q_ref.shape[0] - nq):
        rows.append((residue_ref[...] == fid + r).astype(jnp.float32))
    for f, row in enumerate(rows):
        weight = jnp.sum(pick * row, axis=1, keepdims=True)
        q_ref[f] = jnp.broadcast_to(weight, (nb, nb))


def prepare(at, m, owner, residue, quad, n_freq):
    g, width = m.shape
    nb = width // 2
    whole = lambda *shape: pl.BlockSpec(shape, lambda i: (0,) * len(shape))
    return pl.pallas_call(
        prep_kernel,
        grid=(1,),
        in_specs=[
            pl.BlockSpec(memory_space=pltpu.SMEM),
            whole(g, width),
            whole(1, nb),
            whole(1, nb),
            whole(*quad.shape),
        ],
        out_specs=[whole(2 * nb, 2 * g), whole(n_freq, nb, nb)],
        out_shape=[
            jax.ShapeDtypeStruct((2 * nb, 2 * g), jnp.bfloat16),
            jax.ShapeDtypeStruct((n_freq, nb, nb), jnp.float32),
        ],
        compiler_params=pltpu.CompilerParams(vmem_limit_bytes=8 * 2**20),
        name="prep",
    )(at, m, owner.reshape(1, -1), residue.reshape(1, -1), quad)


def left_kernel(l_ref, q_ref, wir_ref, wii_ref, wrr_ref, wri_ref, *rest, base, blk):
    z_ref = rest[-1]
    g = wir_ref.shape[1]
    nb = q_ref.shape[1]
    n = wir_ref.shape[2]
    total = None
    f = 0
    for re_ref, im_ref in ((wir_ref, wii_ref), (wrr_ref, wri_ref)):
        for k in range(re_ref.shape[0]):
            part = jnp.dot(l_ref[:, :g], re_ref[k], preferred_element_type=jnp.float32)
            part = part + jnp.dot(l_ref[:, g:], im_ref[k], preferred_element_type=jnp.float32)
            weight = jnp.concatenate([q_ref[f]] * (n // nb), axis=1)
            weight = jnp.concatenate([weight, weight], axis=0)
            total = part * weight if total is None else total + part * weight
            f += 1
    hi = total.astype(jnp.bfloat16)
    lo = (total - hi.astype(jnp.float32)).astype(jnp.bfloat16)
    at = (base + pl.program_id(0)) * (n // blk)
    for j in range(n // blk):
        z_ref[at + j, : 2 * nb, :] = hi[:, j * blk : (j + 1) * blk]
        z_ref[at + j, 2 * nb :, :] = lo[:, j * blk : (j + 1) * blk]


def left(l, q, w_imag, w_real, z, base, steps):
    fi, g, width = w_imag.shape
    fr = w_real.shape[0]
    nb = q.shape[1]
    blk = 256
    half = width // 2 // COLS
    re_map = lambda i: (0, 0, base + i)
    im_map = lambda i: (0, 0, base + half + i)
    in_specs = [
        pl.BlockSpec(memory_space=pltpu.VMEM),
        pl.BlockSpec(memory_space=pltpu.VMEM),
        pl.BlockSpec((fi, g, COLS), re_map),
        pl.BlockSpec((fi, g, COLS), im_map),
        pl.BlockSpec((fr, g, COLS), re_map),
        pl.BlockSpec((fr, g, COLS), im_map),
    ]
    args = [l, q, w_imag, w_imag, w_real, w_real]
    aliases = {}
    if z is not None:
        in_specs.append(pl.BlockSpec(memory_space=pltpu.VMEM))
        aliases = {len(args): 0}
        args.append(z)
    shape = (width // 2 // blk, 4 * nb, blk)
    flops = 2 * (fi + fr) * 2 * nb * 2 * g * COLS * steps
    return pl.pallas_call(
        functools.partial(left_kernel, base=base, blk=blk),
        grid=(steps,),
        in_specs=in_specs,
        out_specs=pl.BlockSpec(memory_space=pltpu.VMEM),
        out_shape=pltpu.VMEM(shape, jnp.bfloat16),
        input_output_aliases=aliases,
        cost_estimate=pl.CostEstimate(
            flops=flops, bytes_accessed=2 * (fi + fr) * g * 2 * COLS * steps, transcendentals=0
        ),
        compiler_params=pltpu.CompilerParams(vmem_limit_bytes=32 * 2**20),
    )(*args)


def right_kernel(at_ref, z_ref, *refs, slots, final, seeded):
    refs = list(refs)
    out_ref = refs.pop()
    total = refs.pop(0)[...] if seeded else None
    c, z, y = at_ref[0], at_ref[2], at_ref[3]
    for m_ref, (swapped, far) in zip(refs, slots):
        cls = 1 - c if swapped else c
        for j in range(m_ref.shape[0]):
            near = NEAR[j]
            dz = jnp.where(cls == 0, far, near)
            dy = jnp.where(cls == 0, near, far)
            block = cls * 16 + lax.rem(z - dz + 4, 4) * 4 + lax.rem(y - dy + 4, 4)
            part = jnp.dot(z_ref[block], m_ref[j], preferred_element_type=jnp.float32)
            total = part if total is None else total + part
    if final:
        rows = total.shape[0] // 2
        both = total[:rows] + total[rows:]
        nb = rows // 2
        out_ref[:, :nb] = both[:nb, :nb] - both[nb:, nb:]
        out_ref[:, nb:] = both[:nb, nb:] + both[nb:, :nb]
    else:
        out_ref[...] = total


def stack_kernel(at_ref, own_ref, first_ref, *refs):
    out_ref = refs[-1]
    mine = at_ref[0] == at_ref[1]

    @pl.when(mine)
    def _():
        out_ref[0] = own_ref[...]

    @pl.when(jnp.logical_not(mine))
    def _():
        out_ref[0] = first_ref[...]

    for k, ref in enumerate(refs[:-1]):
        out_ref[k + 1] = ref[...]


def stack(at, own, near):
    return pl.pallas_call(
        stack_kernel,
        in_specs=[pl.BlockSpec(memory_space=pltpu.SMEM)]
        + [pl.BlockSpec(memory_space=pltpu.VMEM) for _ in range(1 + len(near))],
        out_specs=pl.BlockSpec(memory_space=pltpu.VMEM),
        out_shape=jax.ShapeDtypeStruct((len(near),) + own.shape, own.dtype),
        compiler_params=pltpu.CompilerParams(vmem_limit_bytes=4 * 2**20),
        name="stack",
    )(at, own, *near)


def right(at, z, pieces, slots, seed, final):
    rows = z.shape[1]
    shape = (rows // 4, z.shape[2]) if final else (rows, z.shape[2])
    args = [at, z] + ([seed] if seed is not None else []) + list(pieces)
    blocks = sum(p.shape[0] for p in pieces)
    return pl.pallas_call(
        functools.partial(right_kernel, slots=slots, final=final, seeded=seed is not None),
        in_specs=[pl.BlockSpec(memory_space=pltpu.SMEM)]
        + [pl.BlockSpec(memory_space=pltpu.VMEM) for _ in args[1:]],
        out_specs=pl.BlockSpec(memory_space=pltpu.VMEM),
        out_shape=jax.ShapeDtypeStruct(shape, jnp.float32),
        cost_estimate=pl.CostEstimate(
            flops=2 * rows * 256 * 256 * blocks, bytes_accessed=0, transcendentals=0
        ),
        compiler_params=pltpu.CompilerParams(vmem_limit_bytes=24 * 2**20),
        name="right_last" if final else "right_first",
    )(*args)


def on_device(w_imag, w_real, pair_elements, quad_weight, residue_freq, owner_bands):
    bands = pair_elements.shape[1] // 2
    c, xl, z, y = (lax.axis_index(a) for a in ("c", "xl", "z", "y"))
    fid = lax.axis_index(("xh", "c")) * w_real.shape[0]
    at = jnp.stack([c, xl, z, y, fid]).astype(jnp.int32)
    n_freq = w_imag.shape[0] + w_real.shape[0]

    w_real = pltpu.with_memory_space_constraint(w_real, pltpu.HBM)
    w_imag = pltpu.with_memory_space_constraint(w_imag, pltpu.HBM)
    near = []
    for k in NEAR:
        near.append(to_class_core(pair_elements, k))
    l, q = prepare(
        at,
        pair_elements,
        owner_bands,
        residue_freq,
        quad_weight,
        n_freq,
    )
    zl = left(l, q, w_imag, w_real, None, 0, FIRST)
    four = stack(at, pair_elements, near)
    far = []
    for k in FAR[1:]:
        far.append(along_other(four, k))
    zl = left(l, q, w_imag, w_real, zl, FIRST, 8 - FIRST)
    mine = [four] + far
    theirs = []
    for p in mine:
        theirs.append(other_core(p))

    slots = [(s, f) for s in (False, True) for f in FAR]
    first = right(at, zl, mine[:3] + theirs[:3], slots[:3] + slots[4:7], None, False)
    total = right(at, zl, [mine[3], theirs[3]], [slots[3], slots[7]], first, True)

    n_dev = 128
    parts = total.reshape(n_dev, 1, 2 * bands)
    arrived = lax.all_to_all(parts, ALL, split_axis=0, concat_axis=0, tiled=True)
    return arrived.sum(axis=0)


def solution(mesh):
    torus = Mesh(mesh.devices.reshape(2, 2, 2, 4, 4), NAMES)
    freq, gblk = ("xh", "c"), ("xl", "z", "y")
    placed = (
        P(freq, gblk, None),
        P(freq, gblk, None),
        P(gblk, None),
        P(freq, None),
        P(),
        P(),
    )
    return jax.shard_map(
        on_device, mesh=torus, in_specs=placed, out_specs=P(NAMES, None), check_vma=False
    )
```

```python
import functools
import jax
import jax.numpy as jnp
from jax import lax
from jax.experimental import pallas as pl
from jax.experimental.pallas import tpu as pltpu
from jax.sharding import Mesh
from jax.sharding import PartitionSpec as P


NAMES = ("xh", "c", "xl", "z", "y")
PLANE = ("c", "xl", "z", "y")
ALL = NAMES
COLS = 1024
FIRST = 1
NEAR = (0, 1, 3, 2)
FAR = (0, 2, 1, 3)


def device_id(xl, c, z, y):
    return ((c * 2 + xl) * 4 + z % 4) * 4 + y % 4


def moved(x, target):
    pairs = []
    for xl in range(2):
        for c in range(2):
            for z in range(4):
                for y in range(4):
                    to = target(xl, c, z, y)
                    if to is not None:
                        pairs.append((device_id(xl, c, z, y), device_id(*to)))
    return lax.ppermute(x, PLANE, pairs)


def to_class_core(x, k):
    def target(xl, c, z, y):
        if c == xl and k == 0:
            return None
        at = xl if c == xl else 1 - xl
        return (at, xl, z, y + k) if xl == 0 else (at, xl, z + k, y)

    return moved(x, target)


def along_other(x, k):
    return moved(x, lambda xl, c, z, y: (xl, c, z + k, y) if c == 0 else (xl, c, z, y + k))


def other_core(x):
    return moved(x, lambda xl, c, z, y: (xl, 1 - c, z, y))


def prep_kernel(at_ref, m_ref, owner_ref, residue_ref, quad_ref, l_ref, q_ref):
    nb = owner_ref.shape[1]
    owner = jnp.broadcast_to(owner_ref[...].astype(jnp.float32), (nb, nb)).T
    lanes = lax.broadcasted_iota(jnp.int32, (nb, nb), 1)
    pick = (owner.astype(jnp.int32) == lanes).astype(jnp.float32)
    pick16 = pick.astype(jnp.bfloat16)
    nt = (((1,), (1,)), ((), ()))
    g = m_ref.shape[0]
    re = lax.dot_general(pick16, m_ref[:, :nb], nt, preferred_element_type=jnp.float32)
    im = lax.dot_general(pick16, m_ref[:, nb:], nt, preferred_element_type=jnp.float32)
    l_ref[:nb, :g] = re.astype(jnp.bfloat16)
    l_ref[:nb, g:] = im.astype(jnp.bfloat16)
    l_ref[nb:, :g] = (-im).astype(jnp.bfloat16)
    l_ref[nb:, g:] = re.astype(jnp.bfloat16)
    nq = quad_ref.shape[0]
    fid = at_ref[4]
    rows = [quad_ref[f : f + 1, :] for f in range(nq)]
    for r in range(q_ref.shape[0] - nq):
        rows.append((residue_ref[...] == fid + r).astype(jnp.float32))
    for f, row in enumerate(rows):
        weight = jnp.sum(pick * row, axis=1, keepdims=True)
        q_ref[f] = jnp.broadcast_to(weight, (nb, nb))


def prepare(at, m, owner, residue, quad, n_freq):
    g, width = m.shape
    nb = width // 2
    whole = lambda *shape: pl.BlockSpec(shape, lambda i: (0,) * len(shape))
    return pl.pallas_call(
        prep_kernel,
        grid=(1,),
        in_specs=[
            pl.BlockSpec(memory_space=pltpu.SMEM),
            whole(g, width),
            whole(1, nb),
            whole(1, nb),
            whole(*quad.shape),
        ],
        out_specs=[whole(2 * nb, 2 * g), whole(n_freq, nb, nb)],
        out_shape=[
            jax.ShapeDtypeStruct((2 * nb, 2 * g), jnp.bfloat16),
            jax.ShapeDtypeStruct((n_freq, nb, nb), jnp.float32),
        ],
        compiler_params=pltpu.CompilerParams(vmem_limit_bytes=8 * 2**20),
        name="prep",
    )(at, m, owner, residue, quad)


def left_kernel(l_ref, q_ref, wi_ref, wr_ref, *rest, first, chunks):
    z_ref, wi_buf, wr_buf, sem = rest[-4:]
    g, width = wi_ref.shape[1:]
    half = width // 2
    nb = q_ref.shape[1]
    blk = z_ref.shape[2]

    def copies(j):
        col = (first + j) * COLS
        out = []
        for part in range(2):
            for k, (src, buf) in enumerate(((wi_ref, wi_buf), (wr_ref, wr_buf))):
                cols = pl.ds(part * half + col, COLS)
                out.append(
                    pltpu.make_async_copy(
                        src.at[:, :, cols], buf.at[j, part], sem.at[j, 2 * part + k]
                    )
                )
        return out

    for j in range(chunks):
        for copy in copies(j):
            copy.start()

    for j in range(chunks):
        for copy in copies(j):
            copy.wait()
        for s in range(COLS // blk):
            cols = pl.ds(s * blk, blk)
            total = None
            f = 0
            for buf in (wi_buf, wr_buf):
                for k in range(buf.shape[2]):
                    part = jnp.dot(
                        l_ref[:, :g], buf[j, 0, k, :, cols], preferred_element_type=jnp.float32
                    )
                    part = part + jnp.dot(
                        l_ref[:, g:], buf[j, 1, k, :, cols], preferred_element_type=jnp.float32
                    )
                    weight = jnp.concatenate([q_ref[f]] * (blk // nb), axis=1)
                    weight = jnp.concatenate([weight, weight], axis=0)
                    total = part * weight if total is None else total + part * weight
                    f += 1
            hi = total.astype(jnp.bfloat16)
            lo = (total - hi.astype(jnp.float32)).astype(jnp.bfloat16)
            at = (first + j) * (COLS // blk) + s
            z_ref[at, : 2 * nb, :] = hi
            z_ref[at, 2 * nb :, :] = lo


def left(l, q, w_imag, w_real, z, first, chunks):
    fi, g, width = w_imag.shape
    fr = w_real.shape[0]
    nb = q.shape[1]
    blk = 2 * nb
    in_specs = [
        pl.BlockSpec(memory_space=pltpu.VMEM),
        pl.BlockSpec(memory_space=pltpu.VMEM),
        pl.BlockSpec(memory_space=pltpu.HBM),
        pl.BlockSpec(memory_space=pltpu.HBM),
    ]
    args = [l, q, w_imag, w_real]
    aliases = {}
    if z is not None:
        in_specs.append(pl.BlockSpec(memory_space=pltpu.VMEM))
        aliases = {len(args): 0}
        args.append(z)
    shape = (width // 2 // blk, 4 * nb, blk)
    flops = 2 * (fi + fr) * 2 * nb * 2 * g * COLS * chunks
    return pl.pallas_call(
        functools.partial(left_kernel, first=first, chunks=chunks),
        in_specs=in_specs,
        out_specs=pl.BlockSpec(memory_space=pltpu.VMEM),
        out_shape=pltpu.VMEM(shape, jnp.bfloat16),
        input_output_aliases=aliases,
        scratch_shapes=[
            pltpu.VMEM((chunks, 2, fi, g, COLS), jnp.bfloat16),
            pltpu.VMEM((chunks, 2, fr, g, COLS), jnp.bfloat16),
            pltpu.SemaphoreType.DMA((chunks, 4)),
        ],
        cost_estimate=pl.CostEstimate(
            flops=flops, bytes_accessed=4 * (fi + fr) * g * COLS * chunks, transcendentals=0
        ),
        compiler_params=pltpu.CompilerParams(vmem_limit_bytes=34 * 2**20),
    )(*args)


def right_kernel(at_ref, z_ref, *refs, slots, final, seeded):
    refs = list(refs)
    out_ref = refs.pop()
    rows = z_ref.shape[1] // 2
    halves = [slice(0, rows), slice(rows, 2 * rows)]
    seed = refs.pop(0) if seeded else None
    totals = [seed[h] if seeded else None for h in halves]
    c, z, y = at_ref[0], at_ref[2], at_ref[3]
    for m_ref, (swapped, far) in zip(refs, slots):
        cls = 1 - c if swapped else c
        for j in range(m_ref.shape[0]):
            near = NEAR[j]
            dz = jnp.where(cls == 0, far, near)
            dy = jnp.where(cls == 0, near, far)
            block = cls * 16 + lax.rem(z - dz + 4, 4) * 4 + lax.rem(y - dy + 4, 4)
            for i, h in enumerate(halves):
                part = jnp.dot(z_ref[block, h], m_ref[j], preferred_element_type=jnp.float32)
                totals[i] = part if totals[i] is None else totals[i] + part
    if final:
        both = totals[0] + totals[1]
        nb = rows // 2
        out_ref[:, :nb] = both[:nb, :nb] - both[nb:, nb:]
        out_ref[:, nb:] = both[:nb, nb:] + both[nb:, :nb]
    else:
        for i, h in enumerate(halves):
            out_ref[h] = totals[i]


def stack_kernel(at_ref, own_ref, first_ref, *refs):
    out_ref = refs[-1]
    mine = at_ref[0] == at_ref[1]

    @pl.when(mine)
    def _():
        out_ref[0] = own_ref[...]

    @pl.when(jnp.logical_not(mine))
    def _():
        out_ref[0] = first_ref[...]

    for k, ref in enumerate(refs[:-1]):
        out_ref[k + 1] = ref[...]


def stack(at, own, near):
    return pl.pallas_call(
        stack_kernel,
        in_specs=[pl.BlockSpec(memory_space=pltpu.SMEM)]
        + [pl.BlockSpec(memory_space=pltpu.VMEM) for _ in range(1 + len(near))],
        out_specs=pl.BlockSpec(memory_space=pltpu.VMEM),
        out_shape=jax.ShapeDtypeStruct((len(near),) + own.shape, own.dtype),
        compiler_params=pltpu.CompilerParams(vmem_limit_bytes=4 * 2**20),
        name="stack",
    )(at, own, *near)


def right(at, z, pieces, slots, seed, final):
    rows = z.shape[1]
    shape = (rows // 4, z.shape[2]) if final else (rows, z.shape[2])
    args = [at, z] + ([seed] if seed is not None else []) + list(pieces)
    blocks = sum(p.shape[0] for p in pieces)
    return pl.pallas_call(
        functools.partial(right_kernel, slots=slots, final=final, seeded=seed is not None),
        in_specs=[pl.BlockSpec(memory_space=pltpu.SMEM)]
        + [pl.BlockSpec(memory_space=pltpu.VMEM) for _ in args[1:]],
        out_specs=pl.BlockSpec(memory_space=pltpu.VMEM),
        out_shape=jax.ShapeDtypeStruct(shape, jnp.float32),
        cost_estimate=pl.CostEstimate(
            flops=2 * rows * 256 * 256 * blocks, bytes_accessed=0, transcendentals=0
        ),
        compiler_params=pltpu.CompilerParams(vmem_limit_bytes=24 * 2**20),
        name="right_last" if final else "right_first",
    )(*args)


def on_device(w_imag, w_real, pair_elements, quad_weight, residue_freq, owner_bands):
    bands = pair_elements.shape[1] // 2
    c, xl, z, y = (lax.axis_index(a) for a in ("c", "xl", "z", "y"))
    fid = lax.axis_index(("xh", "c")) * w_real.shape[0]
    at = jnp.stack([c, xl, z, y, fid]).astype(jnp.int32)
    n_freq = w_imag.shape[0] + w_real.shape[0]

    in_hbm = lambda x: pltpu.with_memory_space_constraint(x, pltpu.HBM)
    w_imag, w_real = in_hbm(w_imag), in_hbm(w_real)
    near = []
    for k in NEAR:
        near.append(to_class_core(pair_elements, k))
    l, q = prepare(
        at,
        in_hbm(pair_elements),
        in_hbm(owner_bands.reshape(1, -1)),
        in_hbm(residue_freq.reshape(1, -1)),
        in_hbm(quad_weight),
        n_freq,
    )
    zl = left(l, q, w_imag, w_real, None, 0, FIRST)
    four = stack(at, pair_elements, near)
    far = []
    for k in FAR[1:]:
        far.append(along_other(four, k))
    zl = left(l, q, w_imag, w_real, zl, FIRST, 8 - FIRST)
    mine = [four] + far
    theirs = []
    for p in mine:
        theirs.append(other_core(p))

    slots = [(s, f) for s in (False, True) for f in FAR]
    first = right(at, zl, mine + theirs[:1], slots[:5], None, False)
    total = right(at, zl, theirs[1:], slots[5:], first, True)

    n_dev = 128
    parts = total.reshape(n_dev, 1, 2 * bands)
    arrived = lax.all_to_all(parts, ALL, split_axis=0, concat_axis=0, tiled=True)
    return arrived.sum(axis=0)


def solution(mesh):
    torus = Mesh(mesh.devices.reshape(2, 2, 2, 4, 4), NAMES)
    freq, gblk = ("xh", "c"), ("xl", "z", "y")
    placed = (
        P(freq, gblk, None),
        P(freq, gblk, None),
        P(gblk, None),
        P(freq, None),
        P(),
        P(),
    )
    return jax.shard_map(
        on_device, mesh=torus, in_specs=placed, out_specs=P(NAMES, None), check_vma=False
    )
```

```python
import functools
from typing import NamedTuple
import jax
import jax.numpy as jnp
from jax import lax
from jax.experimental import pallas as pl
from jax.experimental.pallas import tpu as pltpu
from jax.sharding import Mesh
from jax.sharding import PartitionSpec as P


NAMES = ("xh", "c", "xl", "z", "y")
PLANE = ("c", "xl", "z", "y")
ALL = NAMES
COLS = 1024
TICK = 40_000_000_000
NEAR = (0, 1, 3, 2)
FAR = (0, 2, 1, 3)


def device_id(xl, c, z, y):
    return ((c * 2 + xl) * 4 + z % 4) * 4 + y % 4


def moved(x, target):
    pairs = []
    for xl in range(2):
        for c in range(2):
            for z in range(4):
                for y in range(4):
                    to = target(xl, c, z, y)
                    if to is not None:
                        pairs.append((device_id(xl, c, z, y), device_id(*to)))
    return lax.ppermute(x, PLANE, pairs)


def to_class_core(x, k):
    def target(xl, c, z, y):
        if c == xl and k == 0:
            return None
        at = xl if c == xl else 1 - xl
        return (at, xl, z, y + k) if xl == 0 else (at, xl, z + k, y)

    return moved(x, target)


def along_other(x, k):
    return moved(x, lambda xl, c, z, y: (xl, c, z + k, y) if c == 0 else (xl, c, z, y + k))


def other_core(x):
    return moved(x, lambda xl, c, z, y: (xl, 1 - c, z, y))


def prep_kernel(tick_ref, m_ref, owner_ref, residue_ref, quad_ref, l_ref, q_ref, copy_ref):
    nb = owner_ref.shape[1]
    owner = jnp.broadcast_to(owner_ref[...].astype(jnp.float32), (nb, nb)).T
    lanes = lax.broadcasted_iota(jnp.int32, (nb, nb), 1)
    copy_ref[...] = m_ref[...]
    pick = (owner.astype(jnp.int32) == lanes).astype(jnp.float32)
    pick16 = pick.astype(jnp.bfloat16)
    nt = (((1,), (1,)), ((), ()))
    g = m_ref.shape[0]
    re = lax.dot_general(pick16, m_ref[:, :nb], nt, preferred_element_type=jnp.float32)
    im = lax.dot_general(pick16, m_ref[:, nb:], nt, preferred_element_type=jnp.float32)
    l_ref[:nb, :g] = re.astype(jnp.bfloat16)
    l_ref[:nb, g:] = im.astype(jnp.bfloat16)
    l_ref[nb:, :g] = (-im).astype(jnp.bfloat16)
    l_ref[nb:, g:] = re.astype(jnp.bfloat16)
    nq = quad_ref.shape[0]
    fid = lax.axis_index(("xh", "c")) * (q_ref.shape[0] - nq)
    rows = [quad_ref[f : f + 1, :] for f in range(nq)]
    for r in range(q_ref.shape[0] - nq):
        rows.append((residue_ref[...] == fid + r).astype(jnp.float32))
    for f, row in enumerate(rows):
        weight = jnp.sum(pick * row, axis=1, keepdims=True)
        q_ref[f] = jnp.broadcast_to(weight, (nb, nb))


def prepare(ticked, m, owner, residue, quad, n_freq):
    g, width = m.shape
    nb = width // 2
    whole = lambda *shape: pl.BlockSpec(shape, lambda i: (0,) * len(shape))
    return pl.pallas_call(
        prep_kernel,
        grid=(1,),
        in_specs=[
            pl.BlockSpec(memory_space=pltpu.VMEM),
            whole(g, width),
            whole(1, nb),
            whole(1, nb),
            whole(*quad.shape),
        ],
        out_specs=[whole(2 * nb, 2 * g), whole(n_freq, nb, nb), whole(g, width)],
        out_shape=[
            jax.ShapeDtypeStruct((2 * nb, 2 * g), jnp.bfloat16),
            jax.ShapeDtypeStruct((n_freq, nb, nb), jnp.float32),
            jax.ShapeDtypeStruct(m.shape, m.dtype),
        ],
        compiler_params=pltpu.CompilerParams(vmem_limit_bytes=8 * 2**20),
        name="prep",
    )(ticked, m, owner, residue, quad)


def left_kernel(*refs, job):
    refs = list(refs)
    l_ref, q_ref, wi_ref, wr_ref = refs[:4]
    sem, buf = refs.pop(), refs.pop() if job.fetched else None
    ahead_ref = refs.pop() if job.ahead else None
    z_ref = refs.pop()
    ready_ref = refs[4] if job.ready else None
    g, width = wi_ref.shape[1:]
    half = width // 2
    nb = q_ref.shape[1]
    blk = z_ref.shape[2]
    c = lax.axis_index("c")

    def base(own):
        return (c if own else 1 - c) * (half // 2)

    def copies(own, chunk, dst, at):
        col = base(own) + chunk * COLS
        return [
            pltpu.make_async_copy(
                wi_ref.at[:, :, pl.ds(pl.multiple_of(part * half + col, COLS), COLS)],
                dst.at[part],
                sem.at[at, part],
            )
            for part in range(2)
        ]

    now = [copies(job.own, job.first + job.ready + j, buf.at[j], j) for j in range(job.fetched)]
    later = [
        copies(job.ahead_own, job.ahead_first + j, ahead_ref.at[j], job.fetched + j)
        for j in range(job.ahead)
    ]
    for pair in now + later:
        for copy in pair:
            copy.start()

    for j in range(job.ready + job.fetched):
        if j < job.ready:
            src = ready_ref.at[j]
        else:
            src = buf.at[j - job.ready]
            for copy in now[j - job.ready]:
                copy.wait()
        for s in range(COLS // blk):
            cols = pl.ds(s * blk, blk)
            col = base(job.own) + (job.first + j) * COLS + s * blk
            pieces = [(src[0, k, :, cols], src[1, k, :, cols]) for k in range(wi_ref.shape[0])]
            pieces += [
                (
                    wr_ref[k, :, pl.ds(pl.multiple_of(col, blk), blk)],
                    wr_ref[k, :, pl.ds(pl.multiple_of(half + col, blk), blk)],
                )
                for k in range(wr_ref.shape[0])
            ]
            total = None
            for f, (re, im) in enumerate(pieces):
                part = jnp.dot(l_ref[:, :g], re, preferred_element_type=jnp.float32)
                part = part + jnp.dot(l_ref[:, g:], im, preferred_element_type=jnp.float32)
                weight = jnp.concatenate([q_ref[f]] * (blk // nb), axis=1)
                weight = jnp.concatenate([weight, weight], axis=0)
                total = part * weight if total is None else total + part * weight
            z_ref[j * (COLS // blk) + s] = total
    for pair in later:
        for copy in pair:
            copy.wait()


class Job(NamedTuple):
    own: bool
    first: int
    ready: int
    fetched: int
    ahead_own: bool = False
    ahead_first: int = 0
    ahead: int = 0


def left(l, q, w_imag, w_real, ready, job):
    fi, g, _ = w_imag.shape
    nb = q.shape[1]
    blk = 2 * nb
    chunks = job.ready + job.fetched
    in_specs = [
        pl.BlockSpec(memory_space=pltpu.VMEM),
        pl.BlockSpec(memory_space=pltpu.VMEM),
        pl.BlockSpec(memory_space=pltpu.HBM),
        pl.BlockSpec(memory_space=pltpu.VMEM),
    ]
    args = [l, q, w_imag, w_real]
    if job.ready:
        in_specs.append(pl.BlockSpec(memory_space=pltpu.VMEM))
        args.append(ready)
    out_shape = [pltpu.VMEM((chunks * COLS // blk, 2 * nb, blk), jnp.float32)]
    if job.ahead:
        out_shape.append(pltpu.VMEM((job.ahead, 2, fi, g, COLS), jnp.bfloat16))
    scratch = [pltpu.SemaphoreType.DMA((job.fetched + job.ahead, 2))]
    if job.fetched:
        scratch.insert(0, pltpu.VMEM((job.fetched, 2, fi, g, COLS), jnp.bfloat16))
    flops = 2 * (fi + w_real.shape[0]) * 2 * nb * 2 * g * COLS * chunks
    return pl.pallas_call(
        functools.partial(left_kernel, job=job),
        in_specs=in_specs,
        out_specs=[pl.BlockSpec(memory_space=pltpu.VMEM) for _ in out_shape],
        out_shape=out_shape,
        scratch_shapes=scratch,
        cost_estimate=pl.CostEstimate(flops=flops, bytes_accessed=0, transcendentals=0),
        compiler_params=pltpu.CompilerParams(vmem_limit_bytes=8 * 2**20),
    )(*args)


def tick_kernel(out_ref):
    out_ref[...] = jnp.zeros_like(out_ref)


def tick():
    return pl.pallas_call(
        tick_kernel,
        out_specs=pl.BlockSpec(memory_space=pltpu.VMEM),
        out_shape=jax.ShapeDtypeStruct((8, 128), jnp.float32),
        cost_estimate=pl.CostEstimate(flops=TICK, bytes_accessed=0, transcendentals=0),
        compiler_params=pltpu.CompilerParams(vmem_limit_bytes=2**20),
        name="tick",
    )()


def products(z_ref, m_refs, fars):
    c, z, y = (lax.axis_index(a) for a in ("c", "z", "y"))
    totals = [None, None]
    for m_ref, far in zip(m_refs, fars):
        blocks = []
        for near in NEAR:
            dz = jnp.where(c == 0, far, near)
            dy = jnp.where(c == 0, near, far)
            blocks.append(lax.rem(z - dz + 4, 4) * 4 + lax.rem(y - dy + 4, 4))
        right_side = jnp.concatenate([m_ref[j] for j in range(m_ref.shape[0])], axis=0)
        for i in range(2):
            left_side = jnp.concatenate([z_ref[i, b] for b in blocks], axis=1)
            part = jnp.dot(left_side, right_side, preferred_element_type=jnp.float32)
            totals[i] = part if totals[i] is None else totals[i] + part
    return totals[0] + totals[1]


def join_kernel(mine_ref, early_ref, late_ref, m_ref, z_ref, sum_ref):
    early = early_ref.shape[0]
    for k in range(mine_ref.shape[0]):
        total = mine_ref[k] + (early_ref[k] if k < early else late_ref[k - early])
        hi = total.astype(jnp.bfloat16)
        z_ref[0, k] = hi
        z_ref[1, k] = (total - hi.astype(jnp.float32)).astype(jnp.bfloat16)
    sum_ref[...] = products(z_ref, [m_ref], FAR[:1])


def right_kernel(z_ref, sum_ref, *refs):
    out_ref = refs[-1]
    nb = out_ref.shape[0]
    both = sum_ref[...] + products(z_ref, refs[:-1], FAR[1:])
    out_ref[:, :nb] = both[:nb, :nb] - both[nb:, nb:]
    out_ref[:, nb:] = both[:nb, nb:] + both[nb:, :nb]


def stack_kernel(source_ref, own_ref, first_ref, *refs):
    del source_ref
    out_ref = refs[-1]
    mine = lax.axis_index("c") == lax.axis_index("xl")

    @pl.when(mine)
    def _():
        out_ref[0] = own_ref[...]

    @pl.when(jnp.logical_not(mine))
    def _():
        out_ref[0] = first_ref[...]

    for k, ref in enumerate(refs[:-1]):
        out_ref[k + 1] = ref[...]


def stack(source, own, near):
    return pl.pallas_call(
        stack_kernel,
        in_specs=[pl.BlockSpec(memory_space=pltpu.HBM)]
        + [pl.BlockSpec(memory_space=pltpu.VMEM) for _ in range(1 + len(near))],
        out_specs=pl.BlockSpec(memory_space=pltpu.VMEM),
        out_shape=jax.ShapeDtypeStruct((len(near),) + own.shape, own.dtype),
        compiler_params=pltpu.CompilerParams(vmem_limit_bytes=4 * 2**20),
        name="stack",
    )(source, own, *near)


def join(mine, early, late, four):
    n, rows, cols = mine.shape
    args = [mine, early, late, four]
    return pl.pallas_call(
        join_kernel,
        in_specs=[pl.BlockSpec(memory_space=pltpu.VMEM) for _ in args],
        out_specs=[pl.BlockSpec(memory_space=pltpu.VMEM) for _ in range(2)],
        out_shape=[
            pltpu.VMEM((2, n, rows, cols), jnp.bfloat16),
            jax.ShapeDtypeStruct((rows, cols), jnp.float32),
        ],
        cost_estimate=pl.CostEstimate(flops=2 * 10**9, bytes_accessed=0, transcendentals=0),
        compiler_params=pltpu.CompilerParams(vmem_limit_bytes=4 * 2**20),
        name="join",
    )(*args)


def right(z, part, pieces):
    rows, cols = part.shape
    args = [z, part] + list(pieces)
    return pl.pallas_call(
        right_kernel,
        in_specs=[pl.BlockSpec(memory_space=pltpu.VMEM) for _ in args],
        out_specs=pl.BlockSpec(memory_space=pltpu.VMEM),
        out_shape=jax.ShapeDtypeStruct((rows // 2, cols), jnp.float32),
        cost_estimate=pl.CostEstimate(flops=2 * 10**9, bytes_accessed=0, transcendentals=0),
        compiler_params=pltpu.CompilerParams(vmem_limit_bytes=4 * 2**20),
        name="right",
    )(*args)


def on_device(w_imag, w_real, pair_elements, quad_weight, residue_freq, owner_bands):
    bands = pair_elements.shape[1] // 2
    n_freq = w_imag.shape[0] + w_real.shape[0]

    in_hbm = lambda x: pltpu.with_memory_space_constraint(x, pltpu.HBM)
    w_imag = in_hbm(w_imag)
    w_real = pltpu.with_memory_space_constraint(w_real, pltpu.VMEM)
    ticked = tick()
    near = []
    for k in NEAR:
        near.append(to_class_core(pair_elements, k))
    l, q, m_here = prepare(
        ticked,
        in_hbm(pair_elements),
        in_hbm(owner_bands.reshape(1, -1)),
        in_hbm(residue_freq.reshape(1, -1)),
        in_hbm(quad_weight),
        n_freq,
    )
    w = (l, q, w_imag, w_real)
    early, ahead = left(*w, None, Job(False, 0, 0, 2, False, 2, 2))
    four = stack(pair_elements, m_here, near)
    far = {}
    for k in FAR[1:]:
        far[k] = along_other(four, k)
    early = other_core(early)
    late, ahead = left(*w, ahead, Job(False, 2, 2, 0, True, 0, 2))
    late = other_core(late)
    (mine,) = left(*w, ahead, Job(True, 0, 2, 2))
    z, part = join(mine, early, late, four)
    total = right(z, part, [far[k] for k in FAR[1:]])

    n_dev = 128
    parts = total.reshape(n_dev, 1, 2 * bands)
    arrived = lax.all_to_all(parts, ALL, split_axis=0, concat_axis=0, tiled=True)
    return arrived.sum(axis=0)


def solution(mesh):
    torus = Mesh(mesh.devices.reshape(2, 2, 2, 4, 4), NAMES)
    freq, gblk = ("xh", "c"), ("xl", "z", "y")
    placed = (
        P(freq, gblk, None),
        P(freq, gblk, None),
        P(gblk, None),
        P(freq, None),
        P(),
        P(),
    )
    return jax.shard_map(
        on_device, mesh=torus, in_specs=placed, out_specs=P(NAMES, None), check_vma=False
    )
```

```python
import functools
from typing import NamedTuple
import jax
import jax.numpy as jnp
from jax import lax
from jax.experimental import pallas as pl
from jax.experimental.pallas import tpu as pltpu
from jax.sharding import Mesh
from jax.sharding import PartitionSpec as P


NAMES = ("xh", "c", "xl", "z", "y")
PLANE = ("c", "xl", "z", "y")
ALL = NAMES
COLS = 1024
TICK = 40_000_000_000
NEAR = (0, 1, 3, 2)


def device_id(xl, c, z, y):
    return ((c * 2 + xl) * 4 + z % 4) * 4 + y % 4


def moved(x, target):
    pairs = []
    for xl in range(2):
        for c in range(2):
            for z in range(4):
                for y in range(4):
                    to = target(xl, c, z, y)
                    if to is not None:
                        pairs.append((device_id(xl, c, z, y), device_id(*to)))
    return lax.ppermute(x, PLANE, pairs)


def to_class_core(x, k):
    def target(xl, c, z, y):
        if c == xl and k == 0:
            return None
        at = xl if c == xl else 1 - xl
        return (at, xl, z, y + k) if xl == 0 else (at, xl, z + k, y)

    return moved(x, target)


def along_other(x, k):
    return moved(x, lambda xl, c, z, y: (xl, c, z + k, y) if c == 0 else (xl, c, z, y + k))


def other_core(x):
    return moved(x, lambda xl, c, z, y: (xl, 1 - c, z, y))


def x_neighbour(x):
    pairs = []
    for xh in range(2):
        for xl in range(2):
            for c in range(2):
                step = 1 if xl == c else -1
                at = (2 * xh + xl + step) % 4
                for z in range(4):
                    for y in range(4):
                        source = (xh * 2 + c) * 32 + (xl * 4 + z) * 4 + y
                        target = (at // 2 * 2 + c) * 32 + (at % 2 * 4 + z) * 4 + y
                        pairs.append((source, target))
    return lax.ppermute(x, ALL, pairs)


def prep_kernel(tick_ref, m_ref, owner_ref, residue_ref, quad_ref, l_ref, q_ref, copy_ref):
    nb = owner_ref.shape[1]
    owner = jnp.broadcast_to(owner_ref[...].astype(jnp.float32), (nb, nb)).T
    lanes = lax.broadcasted_iota(jnp.int32, (nb, nb), 1)
    copy_ref[...] = m_ref[...]
    pick = (owner.astype(jnp.int32) == lanes).astype(jnp.float32)
    pick16 = pick.astype(jnp.bfloat16)
    nt = (((1,), (1,)), ((), ()))
    g = m_ref.shape[0]
    re = lax.dot_general(pick16, m_ref[:, :nb], nt, preferred_element_type=jnp.float32)
    im = lax.dot_general(pick16, m_ref[:, nb:], nt, preferred_element_type=jnp.float32)
    l_ref[:nb, :g] = re.astype(jnp.bfloat16)
    l_ref[:nb, g:] = im.astype(jnp.bfloat16)
    l_ref[nb:, :g] = (-im).astype(jnp.bfloat16)
    l_ref[nb:, g:] = re.astype(jnp.bfloat16)
    nq = quad_ref.shape[0]
    fid = lax.axis_index(("xh", "c")) * (q_ref.shape[0] - nq)
    rows = [quad_ref[f : f + 1, :] for f in range(nq)]
    for r in range(q_ref.shape[0] - nq):
        rows.append((residue_ref[...] == fid + r).astype(jnp.float32))
    for f, row in enumerate(rows):
        weight = jnp.sum(pick * row, axis=1, keepdims=True)
        q_ref[f] = jnp.broadcast_to(weight, (nb, nb))


def prepare(ticked, m, owner, residue, quad, n_freq):
    g, width = m.shape
    nb = width // 2
    whole = lambda *shape: pl.BlockSpec(shape, lambda i: (0,) * len(shape))
    return pl.pallas_call(
        prep_kernel,
        grid=(1,),
        in_specs=[
            pl.BlockSpec(memory_space=pltpu.VMEM),
            whole(g, width),
            whole(1, nb),
            whole(1, nb),
            whole(*quad.shape),
        ],
        out_specs=[whole(2 * nb, 2 * g), whole(n_freq, nb, nb), whole(g, width)],
        out_shape=[
            jax.ShapeDtypeStruct((2 * nb, 2 * g), jnp.bfloat16),
            jax.ShapeDtypeStruct((n_freq, nb, nb), jnp.float32),
            jax.ShapeDtypeStruct(m.shape, m.dtype),
        ],
        compiler_params=pltpu.CompilerParams(vmem_limit_bytes=8 * 2**20),
        name="prep",
    )(ticked, m, owner, residue, quad)


def split(total, z_ref, at):
    hi = total.astype(jnp.bfloat16)
    z_ref[0, at] = hi
    z_ref[1, at] = (total - hi.astype(jnp.float32)).astype(jnp.bfloat16)


def left_kernel(*refs, job):
    refs = list(refs)
    sem = refs.pop()
    buf = refs.pop() if job.fetched else None
    join_ref = refs.pop() if job.joined else None
    ahead_ref = refs.pop() if job.ahead else None
    z_ref = refs.pop()
    l_ref, q_ref, wi_ref, wr_ref = refs[:4]
    refs = refs[4:]
    ready_ref = refs.pop(0) if job.ready else None
    early_ref = refs.pop(0) if job.joined else None
    g, width = wi_ref.shape[1:]
    half = width // 2
    nb = q_ref.shape[1]
    blk = z_ref.shape[2]
    c = lax.axis_index("c")

    def base(own):
        return (c if own else 1 - c) * (half // 2)

    def copies(own, chunk, dst, at):
        col = base(own) + chunk * COLS
        return [
            pltpu.make_async_copy(
                wi_ref.at[:, :, pl.ds(pl.multiple_of(part * half + col, COLS), COLS)],
                dst.at[part],
                sem.at[at, part],
            )
            for part in range(2)
        ]

    now = [copies(job.own, job.first + job.ready + j, buf.at[j], j) for j in range(job.fetched)]
    later = [
        copies(job.ahead_own, job.ahead_first + j, ahead_ref.at[j], job.fetched + j)
        for j in range(job.ahead)
    ]
    for pair in now + later:
        for copy in pair:
            copy.start()

    def chunk(j, src):
        for s in range(COLS // blk):
            cols = pl.ds(s * blk, blk)
            col = base(job.own) + (job.first + j) * COLS + s * blk
            pieces = [(src[0, k, :, cols], src[1, k, :, cols]) for k in range(wi_ref.shape[0])]
            pieces += [
                (
                    wr_ref[k, :, pl.ds(pl.multiple_of(col, blk), blk)],
                    wr_ref[k, :, pl.ds(pl.multiple_of(half + col, blk), blk)],
                )
                for k in range(wr_ref.shape[0])
            ]
            total = None
            for f, (re, im) in enumerate(pieces):
                part = jnp.dot(l_ref[:, :g], re, preferred_element_type=jnp.float32)
                part = part + jnp.dot(l_ref[:, g:], im, preferred_element_type=jnp.float32)
                weight = jnp.concatenate([q_ref[f]] * (blk // nb), axis=1)
                weight = jnp.concatenate([weight, weight], axis=0)
                total = part * weight if total is None else total + part * weight
            at = j * (COLS // blk) + s
            if at < job.joined:
                split(total + early_ref[at], join_ref, at)
            else:
                z_ref[at - job.joined] = total

    for j in range(job.ready + job.fetched):
        if j < job.ready:
            src = ready_ref.at[j]
        else:
            src = buf.at[j - job.ready]
            for copy in now[j - job.ready]:
                copy.wait()

        @pl.when(c >= 0)
        def _(j=j, src=src):
            chunk(j, src)

    for pair in later:
        for copy in pair:
            copy.wait()


class Job(NamedTuple):
    own: bool
    first: int
    ready: int
    fetched: int
    ahead_own: bool = False
    ahead_first: int = 0
    ahead: int = 0
    joined: int = 0


def left(lead, w_imag, w_real, extra, job):
    fi, g, _ = w_imag.shape
    fr = w_real.shape[0]
    nb = g // 2
    blk = 2 * nb
    chunks = job.ready + job.fetched
    blocks = chunks * COLS // blk
    vmem = pl.BlockSpec(memory_space=pltpu.VMEM)
    hbm = pl.BlockSpec(memory_space=pltpu.HBM)
    in_specs = [vmem for _ in lead] + [hbm, vmem] + [vmem for _ in extra]
    args = [*lead, w_imag, w_real, *extra]
    out_shape = [pltpu.VMEM((blocks - job.joined, blk, blk), jnp.float32)]
    scratch = []
    if job.ahead:
        out_shape.append(pltpu.VMEM((job.ahead, 2, fi, g, COLS), jnp.bfloat16))
    if job.joined:
        out_shape.append(pltpu.VMEM((2, blocks, blk, blk), jnp.bfloat16))
    if job.fetched:
        scratch.append(pltpu.VMEM((job.fetched, 2, fi, g, COLS), jnp.bfloat16))
    scratch.append(pltpu.SemaphoreType.DMA((job.fetched + job.ahead, 2)))
    flops = 2 * (fi + fr) * 2 * nb * 2 * g * COLS * chunks
    return pl.pallas_call(
        functools.partial(left_kernel, job=job),
        in_specs=in_specs,
        out_specs=[vmem for _ in out_shape],
        out_shape=out_shape,
        scratch_shapes=scratch,
        cost_estimate=pl.CostEstimate(flops=flops, bytes_accessed=0, transcendentals=0),
        compiler_params=pltpu.CompilerParams(vmem_limit_bytes=8 * 2**20),
    )(*args)


def tick_kernel(out_ref):
    out_ref[...] = jnp.zeros_like(out_ref)


def tick():
    return pl.pallas_call(
        tick_kernel,
        out_specs=pl.BlockSpec(memory_space=pltpu.VMEM),
        out_shape=jax.ShapeDtypeStruct((8, 128), jnp.float32),
        cost_estimate=pl.CostEstimate(flops=TICK, bytes_accessed=0, transcendentals=0),
        compiler_params=pltpu.CompilerParams(vmem_limit_bytes=2**20),
        name="tick",
    )()


def products(z_ref, parts):
    c, z, y = (lax.axis_index(a) for a in ("c", "z", "y"))
    totals = [None, None]
    for m_ref, far, nears in parts:
        blocks = []
        for near in nears:
            dz = jnp.where(c == 0, far, near)
            dy = jnp.where(c == 0, near, far)
            blocks.append(lax.rem(z - dz + 4, 4) * 4 + lax.rem(y - dy + 4, 4))
        right_side = jnp.concatenate([m_ref[j] for j in range(m_ref.shape[0])], axis=0)
        for i in range(2):
            left_side = jnp.concatenate([z_ref[i, b] for b in blocks], axis=1)
            part = jnp.dot(left_side, right_side, preferred_element_type=jnp.float32)
            totals[i] = part if totals[i] is None else totals[i] + part
    return totals[0] + totals[1]


def join_kernel(mine_ref, late_ref, m_ref, z_in_ref, z_ref, sum_ref):
    del z_in_ref
    first = z_ref.shape[1] - mine_ref.shape[0]
    for k in range(mine_ref.shape[0]):
        split(mine_ref[k] + late_ref[k], z_ref, first + k)
    sum_ref[...] = products(z_ref, [(m_ref, 0, NEAR)])


def right_kernel(z_ref, sum_ref, next_ref, last_ref, here_ref, there_ref, out_ref):
    nb = out_ref.shape[0]
    mine = lax.axis_index("c") == lax.axis_index("xl")
    half = here_ref.shape[0]
    lower, upper = NEAR[:half], NEAR[half:]
    here = [jnp.where(mine, a, b) for a, b in zip(lower, upper)]
    there = [jnp.where(mine, b, a) for a, b in zip(lower, upper)]
    parts = [(next_ref, 1, NEAR), (last_ref, 3, NEAR), (here_ref, 2, here), (there_ref, 2, there)]
    both = sum_ref[...] + products(z_ref, parts)
    out_ref[:, :nb] = both[:nb, :nb] - both[nb:, nb:]
    out_ref[:, nb:] = both[:nb, nb:] + both[nb:, :nb]


def stack_kernel(source_ref, own_ref, first_ref, *refs):
    del source_ref
    refs, out_ref, half_ref = refs[:-2], refs[-2], refs[-1]
    mine = lax.axis_index("c") == lax.axis_index("xl")
    half = half_ref.shape[0]

    @pl.when(mine)
    def _():
        out_ref[0] = own_ref[...]
        half_ref[0] = own_ref[...]
        for k in range(1, half):
            half_ref[k] = refs[k - 1][...]

    @pl.when(jnp.logical_not(mine))
    def _():
        out_ref[0] = first_ref[...]
        for k in range(half):
            half_ref[k] = refs[half + k - 1][...]

    for k, ref in enumerate(refs):
        out_ref[k + 1] = ref[...]


def stack(source, own, near):
    return pl.pallas_call(
        stack_kernel,
        in_specs=[pl.BlockSpec(memory_space=pltpu.HBM)]
        + [pl.BlockSpec(memory_space=pltpu.VMEM) for _ in range(1 + len(near))],
        out_specs=[pl.BlockSpec(memory_space=pltpu.VMEM) for _ in range(2)],
        out_shape=[
            jax.ShapeDtypeStruct((n,) + own.shape, own.dtype) for n in (len(near), len(near) // 2)
        ],
        compiler_params=pltpu.CompilerParams(vmem_limit_bytes=4 * 2**20),
        name="stack",
    )(source, own, *near)


def join(mine, late, four, z):
    rows, cols = mine.shape[1:]
    args = [mine, late, four, z]
    return pl.pallas_call(
        join_kernel,
        in_specs=[pl.BlockSpec(memory_space=pltpu.VMEM) for _ in args],
        out_specs=[pl.BlockSpec(memory_space=pltpu.VMEM) for _ in range(2)],
        out_shape=[
            pltpu.VMEM(z.shape, z.dtype),
            jax.ShapeDtypeStruct((rows, cols), jnp.float32),
        ],
        input_output_aliases={3: 0},
        cost_estimate=pl.CostEstimate(flops=2 * 10**9, bytes_accessed=0, transcendentals=0),
        compiler_params=pltpu.CompilerParams(vmem_limit_bytes=4 * 2**20),
        name="join",
    )(*args)


def right(z, part, pieces):
    rows, cols = part.shape
    args = [z, part] + list(pieces)
    return pl.pallas_call(
        right_kernel,
        in_specs=[pl.BlockSpec(memory_space=pltpu.VMEM) for _ in args],
        out_specs=pl.BlockSpec(memory_space=pltpu.VMEM),
        out_shape=jax.ShapeDtypeStruct((rows // 2, cols), jnp.float32),
        cost_estimate=pl.CostEstimate(flops=2 * 10**9, bytes_accessed=0, transcendentals=0),
        compiler_params=pltpu.CompilerParams(vmem_limit_bytes=4 * 2**20),
        name="right",
    )(*args)


def on_device(w_imag, w_real, pair_elements, quad_weight, residue_freq, owner_bands):
    bands = pair_elements.shape[1] // 2

    in_hbm = lambda x: pltpu.with_memory_space_constraint(x, pltpu.HBM)
    w_imag = in_hbm(w_imag)
    w_real = pltpu.with_memory_space_constraint(w_real, pltpu.VMEM)
    ticked = tick()
    near = []
    for k in NEAR:
        near.append(to_class_core(pair_elements, k))
    n_freq = w_imag.shape[0] + w_real.shape[0]
    l, q, m_here = prepare(
        ticked,
        in_hbm(pair_elements),
        in_hbm(owner_bands.reshape(1, -1)),
        in_hbm(residue_freq.reshape(1, -1)),
        in_hbm(quad_weight),
        n_freq,
    )
    w = ((l, q), w_imag, w_real)
    early, ahead = left(*w, [], Job(False, 0, 0, 2, False, 2, 2))
    four, half = stack(pair_elements, m_here, near)
    here = along_other(half, 2)
    next_far = along_other(four, 1)
    last_far = along_other(four, 3)
    early = other_core(early)
    late, ahead = left(*w, [ahead], Job(False, 2, 2, 0, True, 0, 2))
    late = other_core(late)
    there = x_neighbour(here)
    mine, z = left(*w, [ahead, early], Job(True, 0, 2, 2, joined=early.shape[0]))
    z, part = join(mine, late, four, z)
    total = right(z, part, [next_far, last_far, here, there])

    n_dev = 128
    parts = total.reshape(n_dev, 1, 2 * bands)
    arrived = lax.all_to_all(parts, ALL, split_axis=0, concat_axis=0, tiled=True)
    return arrived.sum(axis=0)


def solution(mesh):
    torus = Mesh(mesh.devices.reshape(2, 2, 2, 4, 4), NAMES)
    freq, gblk = ("xh", "c"), ("xl", "z", "y")
    placed = (
        P(freq, gblk, None),
        P(freq, gblk, None),
        P(gblk, None),
        P(freq, None),
        P(),
        P(),
    )
    return jax.shard_map(
        on_device, mesh=torus, in_specs=placed, out_specs=P(NAMES, None), check_vma=False
    )
```

```python
import functools
from typing import NamedTuple
import jax
import jax.numpy as jnp
from jax import lax
from jax.experimental import pallas as pl
from jax.experimental.pallas import tpu as pltpu
from jax.sharding import Mesh
from jax.sharding import PartitionSpec as P


NAMES = ("xh", "c", "xl", "z", "y")
PLANE = ("c", "xl", "z", "y")
ALL = NAMES
COLS = 1024
TICK = 40_000_000_000
NEAR = (0, 1, 3, 2)


def device_id(xl, c, z, y):
    return ((c * 2 + xl) * 4 + z % 4) * 4 + y % 4


def moved(x, target):
    pairs = []
    for xl in range(2):
        for c in range(2):
            for z in range(4):
                for y in range(4):
                    to = target(xl, c, z, y)
                    if to is not None:
                        pairs.append((device_id(xl, c, z, y), device_id(*to)))
    return lax.ppermute(x, PLANE, pairs)


def to_class_core(x, k):
    def target(xl, c, z, y):
        if c == xl and k == 0:
            return None
        at = xl if c == xl else 1 - xl
        return (at, xl, z, y + k) if xl == 0 else (at, xl, z + k, y)

    return moved(x, target)


def along_other(x, k):
    return moved(x, lambda xl, c, z, y: (xl, c, z + k, y) if c == 0 else (xl, c, z, y + k))


def other_core(x):
    return moved(x, lambda xl, c, z, y: (xl, 1 - c, z, y))


def x_neighbour(x):
    pairs = []
    for xh in range(2):
        for xl in range(2):
            for c in range(2):
                step = 1 if xl == c else -1
                at = (2 * xh + xl + step) % 4
                for z in range(4):
                    for y in range(4):
                        source = (xh * 2 + c) * 32 + (xl * 4 + z) * 4 + y
                        target = (at // 2 * 2 + c) * 32 + (at % 2 * 4 + z) * 4 + y
                        pairs.append((source, target))
    return lax.ppermute(x, ALL, pairs)


def prep_kernel(tick_ref, m_ref, owner_ref, residue_ref, quad_ref, l_ref, q_ref, copy_ref):
    nb = owner_ref.shape[1]
    owner = jnp.broadcast_to(owner_ref[...].astype(jnp.float32), (nb, nb)).T
    lanes = lax.broadcasted_iota(jnp.int32, (nb, nb), 1)
    copy_ref[...] = m_ref[...]
    pick = (owner.astype(jnp.int32) == lanes).astype(jnp.float32)
    pick16 = pick.astype(jnp.bfloat16)
    nt = (((1,), (1,)), ((), ()))
    g = m_ref.shape[0]
    re = lax.dot_general(pick16, m_ref[:, :nb], nt, preferred_element_type=jnp.float32)
    im = lax.dot_general(pick16, m_ref[:, nb:], nt, preferred_element_type=jnp.float32)
    l_ref[:nb, :g] = re.astype(jnp.bfloat16)
    l_ref[:nb, g:] = im.astype(jnp.bfloat16)
    l_ref[nb:, :g] = (-im).astype(jnp.bfloat16)
    l_ref[nb:, g:] = re.astype(jnp.bfloat16)
    nq = quad_ref.shape[0]
    fid = lax.axis_index(("xh", "c")) * (q_ref.shape[0] - nq)
    rows = [quad_ref[f : f + 1, :] for f in range(nq)]
    for r in range(q_ref.shape[0] - nq):
        rows.append((residue_ref[...] == fid + r).astype(jnp.float32))
    for f, row in enumerate(rows):
        weight = jnp.sum(pick * row, axis=1, keepdims=True)
        q_ref[f] = jnp.broadcast_to(weight, (nb, nb))


def prepare(ticked, m, owner, residue, quad, n_freq):
    g, width = m.shape
    nb = width // 2
    whole = lambda *shape: pl.BlockSpec(shape, lambda i: (0,) * len(shape))
    return pl.pallas_call(
        prep_kernel,
        grid=(1,),
        in_specs=[
            pl.BlockSpec(memory_space=pltpu.VMEM),
            whole(g, width),
            whole(1, nb),
            whole(1, nb),
            whole(*quad.shape),
        ],
        out_specs=[whole(2 * nb, 2 * g), whole(n_freq, nb, nb), whole(g, width)],
        out_shape=[
            jax.ShapeDtypeStruct((2 * nb, 2 * g), jnp.bfloat16),
            jax.ShapeDtypeStruct((n_freq, nb, nb), jnp.float32),
            jax.ShapeDtypeStruct(m.shape, m.dtype),
        ],
        compiler_params=pltpu.CompilerParams(vmem_limit_bytes=8 * 2**20),
        name="prep",
    )(ticked, m, owner, residue, quad)


def split(total, z_ref, at):
    hi = total.astype(jnp.bfloat16)
    z_ref[0, at] = hi
    z_ref[1, at] = (total - hi.astype(jnp.float32)).astype(jnp.bfloat16)


def left_kernel(*refs, job):
    refs = list(refs)
    sem = refs.pop()
    buf = refs.pop() if job.fetched else None
    join_ref = refs.pop() if job.joined else None
    ahead_ref = refs.pop() if job.ahead else None
    z_ref = refs.pop()
    l_ref, q_ref, wi_ref, wr_ref = refs[:4]
    refs = refs[4:]
    ready_ref = refs.pop(0) if job.ready else None
    early_ref = refs.pop(0) if job.joined else None
    g, width = wi_ref.shape[1:]
    half = width // 2
    nb = q_ref.shape[1]
    blk = z_ref.shape[2]
    c = lax.axis_index("c")

    def base(own):
        return (c if own else 1 - c) * (half // 2)

    def copies(own, chunk, dst, at):
        col = base(own) + chunk * COLS
        return [
            pltpu.make_async_copy(
                wi_ref.at[:, :, pl.ds(pl.multiple_of(part * half + col, COLS), COLS)],
                dst.at[part],
                sem.at[at, part],
            )
            for part in range(2)
        ]

    now = [copies(job.own, job.first + job.ready + j, buf.at[j], j) for j in range(job.fetched)]
    later = [
        copies(job.ahead_own, job.ahead_first + j, ahead_ref.at[j], job.fetched + j)
        for j in range(job.ahead)
    ]
    for pair in now + later:
        for copy in pair:
            copy.start()

    def chunk(j, src):
        for s in range(COLS // blk):
            cols = pl.ds(s * blk, blk)
            col = base(job.own) + (job.first + j) * COLS + s * blk
            pieces = [(src[0, k, :, cols], src[1, k, :, cols]) for k in range(wi_ref.shape[0])]
            pieces += [
                (
                    wr_ref[k, :, pl.ds(pl.multiple_of(col, blk), blk)],
                    wr_ref[k, :, pl.ds(pl.multiple_of(half + col, blk), blk)],
                )
                for k in range(wr_ref.shape[0])
            ]
            total = None
            for f, (re, im) in enumerate(pieces):
                part = jnp.dot(l_ref[:, :g], re, preferred_element_type=jnp.float32)
                part = part + jnp.dot(l_ref[:, g:], im, preferred_element_type=jnp.float32)
                weight = jnp.concatenate([q_ref[f]] * (blk // nb), axis=1)
                weight = jnp.concatenate([weight, weight], axis=0)
                total = part * weight if total is None else total + part * weight
            at = j * (COLS // blk) + s
            if at < job.joined:
                split(total + early_ref[at], join_ref, at)
            else:
                z_ref[at - job.joined] = total

    for j in range(job.ready + job.fetched):
        if j < job.ready:
            src = ready_ref.at[j]
        else:
            src = buf.at[j - job.ready]
            for copy in now[j - job.ready]:
                copy.wait()

        @pl.when(c >= 0)
        def _(j=j, src=src):
            chunk(j, src)

    for pair in later:
        for copy in pair:
            copy.wait()


class Job(NamedTuple):
    own: bool
    first: int
    ready: int
    fetched: int
    ahead_own: bool = False
    ahead_first: int = 0
    ahead: int = 0
    joined: int = 0


def left(lead, w_imag, w_real, extra, job):
    fi, g, _ = w_imag.shape
    fr = w_real.shape[0]
    nb = g // 2
    blk = 2 * nb
    chunks = job.ready + job.fetched
    blocks = chunks * COLS // blk
    vmem = pl.BlockSpec(memory_space=pltpu.VMEM)
    hbm = pl.BlockSpec(memory_space=pltpu.HBM)
    in_specs = [vmem for _ in lead] + [hbm, vmem] + [vmem for _ in extra]
    args = [*lead, w_imag, w_real, *extra]
    out_shape = [pltpu.VMEM((blocks - job.joined, blk, blk), jnp.float32)]
    scratch = []
    if job.ahead:
        out_shape.append(pltpu.VMEM((job.ahead, 2, fi, g, COLS), jnp.bfloat16))
    if job.joined:
        out_shape.append(pltpu.VMEM((2, blocks, blk, blk), jnp.bfloat16))
    if job.fetched:
        scratch.append(pltpu.VMEM((job.fetched, 2, fi, g, COLS), jnp.bfloat16))
    scratch.append(pltpu.SemaphoreType.DMA((job.fetched + job.ahead, 2)))
    flops = 2 * (fi + fr) * 2 * nb * 2 * g * COLS * chunks
    return pl.pallas_call(
        functools.partial(left_kernel, job=job),
        in_specs=in_specs,
        out_specs=[vmem for _ in out_shape],
        out_shape=out_shape,
        scratch_shapes=scratch,
        cost_estimate=pl.CostEstimate(flops=flops, bytes_accessed=0, transcendentals=0),
        compiler_params=pltpu.CompilerParams(vmem_limit_bytes=8 * 2**20),
    )(*args)


def tick_kernel(out_ref):
    out_ref[...] = jnp.zeros_like(out_ref)


def tick():
    return pl.pallas_call(
        tick_kernel,
        out_specs=pl.BlockSpec(memory_space=pltpu.VMEM),
        out_shape=jax.ShapeDtypeStruct((8, 128), jnp.float32),
        cost_estimate=pl.CostEstimate(flops=TICK, bytes_accessed=0, transcendentals=0),
        compiler_params=pltpu.CompilerParams(vmem_limit_bytes=2**20),
        name="tick",
    )()


def products(z_ref, parts):
    c, z, y = (lax.axis_index(a) for a in ("c", "z", "y"))
    totals = [None, None]
    for m_ref, far, nears in parts:
        blocks = []
        for near in nears:
            dz = jnp.where(c == 0, far, near)
            dy = jnp.where(c == 0, near, far)
            blocks.append(lax.rem(z - dz + 4, 4) * 4 + lax.rem(y - dy + 4, 4))
        right_side = jnp.concatenate([m_ref[j] for j in range(m_ref.shape[0])], axis=0)
        for i in range(2):
            left_side = jnp.concatenate([z_ref[i, b] for b in blocks], axis=1)
            part = jnp.dot(left_side, right_side, preferred_element_type=jnp.float32)
            totals[i] = part if totals[i] is None else totals[i] + part
    return totals[0] + totals[1]


def join_kernel(mine_ref, late_ref, m_ref, z_in_ref, z_ref, sum_ref):
    del z_in_ref
    first = z_ref.shape[1] - mine_ref.shape[0]
    for k in range(mine_ref.shape[0]):
        split(mine_ref[k] + late_ref[k], z_ref, first + k)
    sum_ref[...] = products(z_ref, [(m_ref, 0, NEAR)])


def right_kernel(z_ref, sum_ref, next_ref, last_ref, here_ref, there_ref, out_ref):
    nb = out_ref.shape[0]
    mine = lax.axis_index("c") == lax.axis_index("xl")
    half = here_ref.shape[0]
    lower, upper = NEAR[:half], NEAR[half:]
    here = [jnp.where(mine, a, b) for a, b in zip(lower, upper)]
    there = [jnp.where(mine, b, a) for a, b in zip(lower, upper)]
    parts = [(next_ref, 1, NEAR), (last_ref, 3, NEAR), (here_ref, 2, here), (there_ref, 2, there)]
    both = sum_ref[...] + products(z_ref, parts)
    out_ref[:, :nb] = both[:nb, :nb] - both[nb:, nb:]
    out_ref[:, nb:] = both[:nb, nb:] + both[nb:, :nb]


def stack_kernel(source_ref, own_ref, first_ref, *refs):
    del source_ref
    refs, out_ref, half_ref = refs[:-2], refs[-2], refs[-1]
    mine = lax.axis_index("c") == lax.axis_index("xl")
    half = half_ref.shape[0]

    @pl.when(mine)
    def _():
        out_ref[0] = own_ref[...]
        half_ref[0] = own_ref[...]
        for k in range(1, half):
            half_ref[k] = refs[k - 1][...]

    @pl.when(jnp.logical_not(mine))
    def _():
        out_ref[0] = first_ref[...]
        for k in range(half):
            half_ref[k] = refs[half + k - 1][...]

    for k, ref in enumerate(refs):
        out_ref[k + 1] = ref[...]


def stack(source, own, near):
    return pl.pallas_call(
        stack_kernel,
        in_specs=[pl.BlockSpec(memory_space=pltpu.HBM)]
        + [pl.BlockSpec(memory_space=pltpu.VMEM) for _ in range(1 + len(near))],
        out_specs=[pl.BlockSpec(memory_space=pltpu.VMEM) for _ in range(2)],
        out_shape=[
            jax.ShapeDtypeStruct((n,) + own.shape, own.dtype) for n in (len(near), len(near) // 2)
        ],
        compiler_params=pltpu.CompilerParams(vmem_limit_bytes=4 * 2**20),
        name="stack",
    )(source, own, *near)


def join(mine, late, four, z):
    rows, cols = mine.shape[1:]
    args = [mine, late, four, z]
    return pl.pallas_call(
        join_kernel,
        in_specs=[pl.BlockSpec(memory_space=pltpu.VMEM) for _ in args],
        out_specs=[pl.BlockSpec(memory_space=pltpu.VMEM) for _ in range(2)],
        out_shape=[
            pltpu.VMEM(z.shape, z.dtype),
            jax.ShapeDtypeStruct((rows, cols), jnp.float32),
        ],
        input_output_aliases={3: 0},
        cost_estimate=pl.CostEstimate(flops=2 * 10**9, bytes_accessed=0, transcendentals=0),
        compiler_params=pltpu.CompilerParams(vmem_limit_bytes=4 * 2**20),
        name="join",
    )(*args)


def right(z, part, pieces):
    rows, cols = part.shape
    args = [z, part] + list(pieces)
    return pl.pallas_call(
        right_kernel,
        in_specs=[pl.BlockSpec(memory_space=pltpu.VMEM) for _ in args],
        out_specs=pl.BlockSpec(memory_space=pltpu.VMEM),
        out_shape=jax.ShapeDtypeStruct((rows // 2, cols), jnp.float32),
        cost_estimate=pl.CostEstimate(flops=2 * 10**9, bytes_accessed=0, transcendentals=0),
        compiler_params=pltpu.CompilerParams(vmem_limit_bytes=4 * 2**20),
        name="right",
    )(*args)


def add_up_kernel(parts_ref, out_ref):
    out_ref[...] = jnp.sum(parts_ref[...], axis=0)


def add_up(parts):
    return pl.pallas_call(
        add_up_kernel,
        in_specs=[pl.BlockSpec(memory_space=pltpu.VMEM)],
        out_specs=pl.BlockSpec(memory_space=pltpu.VMEM),
        out_shape=jax.ShapeDtypeStruct(parts.shape[1:], parts.dtype),
        compiler_params=pltpu.CompilerParams(vmem_limit_bytes=4 * 2**20),
        name="add_up",
    )(parts)


def on_device(w_imag, w_real, pair_elements, quad_weight, residue_freq, owner_bands):
    bands = pair_elements.shape[1] // 2

    in_hbm = lambda x: pltpu.with_memory_space_constraint(x, pltpu.HBM)
    w_imag = in_hbm(w_imag)
    w_real = pltpu.with_memory_space_constraint(w_real, pltpu.VMEM)
    ticked = tick()
    near = []
    for k in NEAR:
        near.append(to_class_core(pair_elements, k))
    n_freq = w_imag.shape[0] + w_real.shape[0]
    l, q, m_here = prepare(
        ticked,
        in_hbm(pair_elements),
        in_hbm(owner_bands.reshape(1, -1)),
        in_hbm(residue_freq.reshape(1, -1)),
        in_hbm(quad_weight),
        n_freq,
    )
    w = ((l, q), w_imag, w_real)
    early, ahead = left(*w, [], Job(False, 0, 0, 2, False, 2, 2))
    four, half = stack(pair_elements, m_here, near)
    here = along_other(half, 2)
    next_far = along_other(four, 1)
    last_far = along_other(four, 3)
    early = other_core(early)
    late, ahead = left(*w, [ahead], Job(False, 2, 2, 0, True, 0, 2))
    late = other_core(late)
    there = x_neighbour(here)
    mine, z = left(*w, [ahead, early], Job(True, 0, 2, 2, joined=early.shape[0]))
    z, part = join(mine, late, four, z)
    total = right(z, part, [next_far, last_far, here, there])

    n_dev = 128
    parts = total.reshape(n_dev, 1, 2 * bands)
    arrived = lax.all_to_all(parts, ALL, split_axis=0, concat_axis=0, tiled=True)
    return add_up(arrived)


def solution(mesh):
    torus = Mesh(mesh.devices.reshape(2, 2, 2, 4, 4), NAMES)
    freq, gblk = ("xh", "c"), ("xl", "z", "y")
    placed = (
        P(freq, gblk, None),
        P(freq, gblk, None),
        P(gblk, None),
        P(freq, None),
        P(),
        P(),
    )
    return jax.shard_map(
        on_device, mesh=torus, in_specs=placed, out_specs=P(NAMES, None), check_vma=False
    )
```
